16 devices in a mesh: rep: 1, dp: 16 (over x, y, z, core).
Axes of the slice: x: 2, y: 2, z: 2, core: 2. Of those that a mesh axis runs over, the one named last changes fastest.
Arguments:
- x: bfloat16 [16, 2048, 1024], P(('rep', 'dp'))
- dy: bfloat16 [16, 2048, 1024], P(('rep', 'dp'))
- wq: bfloat16 [2, 1024, 1024], replicated
- wk: bfloat16 [2, 1024, 1024], replicated
- wv: bfloat16 [2, 1024, 1024], replicated
- wo: bfloat16 [2, 1024, 1024], replicated
- w_gate: bfloat16 [2, 1024, 4096], replicated
- w_up: bfloat16 [2, 1024, 4096], replicated
- w_down: bfloat16 [2, 4096, 1024], replicated
- m_wq: float32 [2, 1024, 1024], P(None, 'dp')
- m_wk: float32 [2, 1024, 1024], P(None, 'dp')
- m_wv: float32 [2, 1024, 1024], P(None, 'dp')
- m_wo: float32 [2, 1024, 1024], P(None, 'dp')
- m_w_gate: float32 [2, 1024, 4096], P(None, 'dp')
- m_w_up: float32 [2, 1024, 4096], P(None, 'dp')
- m_w_down: float32 [2, 4096, 1024], P(None, 'dp')
- v_wq: float32 [2, 1024, 1024], P(None, 'dp')
- v_wk: float32 [2, 1024, 1024], P(None, 'dp')
- v_wv: float32 [2, 1024, 1024], P(None, 'dp')
- v_wo: float32 [2, 1024, 1024], P(None, 'dp')
- v_w_gate: float32 [2, 1024, 4096], P(None, 'dp')
- v_w_up: float32 [2, 1024, 4096], P(None, 'dp')
- v_w_down: float32 [2, 4096, 1024], P(None, 'dp')
Outputs:
- output 1: bfloat16 [2, 1024, 1024], P('rep')
- output 2: bfloat16 [2, 1024, 1024], P('rep')
- output 3: bfloat16 [2, 1024, 1024], P('rep')
- output 4: bfloat16 [2, 1024, 1024], P('rep')
- output 5: bfloat16 [2, 1024, 4096], P('rep')
- output 6: bfloat16 [2, 1024, 4096], P('rep')
- output 7: bfloat16 [2, 4096, 1024], P('rep')
- output 8: float32 [2, 1024, 1024], P('rep', 'dp')
- output 9: float32 [2, 1024, 1024], P('rep', 'dp')
- output 10: float32 [2, 1024, 1024], P('rep', 'dp')
- output 11: float32 [2, 1024, 1024], P('rep', 'dp')
- output 12: float32 [2, 1024, 4096], P('rep', 'dp')
- output 13: float32 [2, 1024, 4096], P('rep', 'dp')
- output 14: float32 [2, 4096, 1024], P('rep', 'dp')
- output 15: float32 [2, 1024, 1024], P('rep', 'dp')
- output 16: float32 [2, 1024, 1024], P('rep', 'dp')
- output 17: float32 [2, 1024, 1024], P('rep', 'dp')
- output 18: float32 [2, 1024, 1024], P('rep', 'dp')
- output 19: float32 [2, 1024, 4096], P('rep', 'dp')
- output 20: float32 [2, 1024, 4096], P('rep', 'dp')
- output 21: float32 [2, 4096, 1024], P('rep', 'dp')
All inputs are finite; a program needn't handle non-finite values.
Results may differ from the reference program's by a relative error of at most 0.0251.
Values are sent between devices in bfloat16 or wider.
A program may use at most 2 GiB of HBM per device.

```python
import jax
import jax.numpy as jnp
from jax import lax

SEQUENCES = 16
TOKENS = 2048
D = 1024
HEADS = 4
KV_HEADS = 4
HEAD = 256
FF = 4096
LAYERS = 2
THETA = 10000
NAMES = ("wq", "wk", "wv", "wo", "w_gate", "w_up", "w_down")
SHAPES = {
    "wq": (LAYERS, D, HEADS * HEAD),
    "wk": (LAYERS, D, KV_HEADS * HEAD),
    "wv": (LAYERS, D, KV_HEADS * HEAD),
    "wo": (LAYERS, HEADS * HEAD, D),
    "w_gate": (LAYERS, D, FF),
    "w_up": (LAYERS, D, FF),
    "w_down": (LAYERS, FF, D),
}


def bump(key, n, height):
    away = (jnp.arange(n, dtype=jnp.int32) - jax.random.randint(key, (), 0, n, jnp.int32)) % n
    return jnp.where(away < n // 8, height, 1.0)


def together(key, own, strength):
    shared = jax.random.normal(key, own.shape[1:], jnp.float32)
    return (own + strength * shared) * lax.rsqrt(1 + strength * strength)


def setup_inputs(seed: int = 0, part: int = 0) -> dict:
    kx, kdy, ka, kb, kz, kf, kh, kl, *keys = jax.random.split(jax.random.key(seed), 8 + 3 * len(NAMES))
    kx, kdy, ka, kb = (jax.random.fold_in(k, part) for k in (kx, kdy, ka, kb))
    kw, km, kv = (keys[i::3] for i in range(3))
    shape = (SEQUENCES, TOKENS, D)
    much_x, much_dy = jax.random.uniform(kz, (2,), jnp.float32, 0.0, 1.0)
    loud = 2.0 ** jax.random.uniform(jax.random.fold_in(kz, 1), (), jnp.float32, -1.0, 2.0)
    layers = 2.0 ** jax.random.uniform(kl, (LAYERS, 1, 1), jnp.float32, -1.0, 1.0)
    times = {"wq": 1.0, "wk": 1.0, "wv": 2.0, "wo": layers, "w_gate": 1.0, "w_up": bump(kh, FF, 4.0), "w_down": layers}
    x = together(ka, jax.random.normal(kx, shape, jnp.float32), much_x) * bump(kf, D, 4.0)
    dy = together(kb, jax.random.normal(kdy, shape, jnp.float32), much_dy)
    drawn = {"x": x.astype(jnp.bfloat16), "dy": (loud * dy * (SEQUENCES * TOKENS) ** -0.5).astype(jnp.bfloat16)}
    for key, name in zip(kw, NAMES, strict=True):
        drawn[name] = (jax.random.normal(key, SHAPES[name], jnp.float32) * SHAPES[name][1] ** -0.5 * times[name]).astype(jnp.bfloat16)
    for key, name in zip(km, NAMES, strict=True):
        drawn[f"m_{name}"] = 0.1 * jax.random.normal(key, SHAPES[name], jnp.float32)
    for key, name in zip(kv, NAMES, strict=True):
        drawn[f"v_{name}"] = jax.random.uniform(key, SHAPES[name], jnp.float32, 0.02, 0.06)
    return drawn


def matmul(a, w):
    return jnp.dot(a, w, preferred_element_type=jnp.float32).astype(jnp.bfloat16)


def normed(h):
    wide = h.astype(jnp.float32)
    scale = lax.rsqrt(jnp.mean(wide**2, -1, keepdims=True) + 1e-6)
    return (wide * scale).astype(jnp.bfloat16)


def turned(t, theta):
    half = t.shape[-1] // 2
    angle = jnp.arange(t.shape[0], dtype=jnp.float32)[:, None] * theta ** (-jnp.arange(half, dtype=jnp.float32) / half)
    cos, sin = jnp.cos(angle)[:, None], jnp.sin(angle)[:, None]
    a, b = t[..., :half].astype(jnp.float32), t[..., half:].astype(jnp.float32)
    return jnp.concatenate([a * cos - b * sin, b * cos + a * sin], -1).astype(jnp.bfloat16)


def seen_by(q, k, v):
    tokens, kv = q.shape[0], k.shape[1]
    q = q.reshape(tokens, kv, -1, q.shape[-1])
    scores = jnp.einsum("tgsd,ugd->gstu", q.astype(jnp.float32), k.astype(jnp.float32)) * q.shape[-1] ** -0.5
    place = jnp.arange(tokens)
    weights = jax.nn.softmax(jnp.where(place[:, None] >= place, scores, -jnp.inf), -1).astype(jnp.bfloat16)
    return jnp.einsum("gstu,ugd->tgsd", weights.astype(jnp.float32), v.astype(jnp.float32)).astype(jnp.bfloat16).reshape(tokens, -1)


def layer(h, w):
    a = normed(h)
    q, k = (turned(matmul(a, w[name]).reshape(h.shape[0], -1, HEAD), THETA) for name in ("wq", "wk"))
    h = h + matmul(seen_by(q, k, matmul(a, w["wv"]).reshape(h.shape[0], -1, HEAD)), w["wo"])
    b = normed(h)
    gate = jnp.dot(b, w["w_gate"], preferred_element_type=jnp.float32)
    up = jnp.dot(b, w["w_up"], preferred_element_type=jnp.float32)
    return h + matmul((jax.nn.silu(gate) * up).astype(jnp.bfloat16), w["w_down"])


def adamw(w, m, v, g):
    m = 0.9 * m + 0.1 * g
    v = 0.95 * v + 0.05 * g * g
    step = m * lax.rsqrt(v + 1e-8) + 0.1 * w
    return (w - 0.02 * step).astype(jnp.bfloat16), m, v


def clipped(gradients, sum_of_squares, count):
    factor = jnp.minimum(1.0, 0.5 * lax.rsqrt(sum_of_squares / count + 1e-30))
    return [g * factor for g in gradients]


def stack(weights, h):
    return lax.scan(lambda h, w: (layer(h, w), None), h, weights)[0]


def reference(x, dy, wq, wk, wv, wo, w_gate, w_up, w_down, m_wq, m_wk, m_wv, m_wo, m_w_gate, m_w_up, m_w_down, v_wq, v_wk, v_wv, v_wo, v_w_gate, v_w_up, v_w_down):
    weights = dict(zip(NAMES, (wq, wk, wv, wo, w_gate, w_up, w_down), strict=True))

    def take(so_far, sequence):
        h, by_y = sequence
        _, back = jax.vjp(stack, weights, h)
        by_weights, by_h = back(by_y)
        return jax.tree.map(lambda total, term: total + term.astype(jnp.float32), so_far, by_weights), by_h

    none_yet = {name: jnp.zeros(w.shape, jnp.float32) for name, w in weights.items()}
    by_weights, by_x = lax.scan(take, none_yet, (x, dy))
    gradients = [by_weights[name].astype(jnp.bfloat16).astype(jnp.float32) for name in NAMES]
    gradients = clipped(gradients, sum(jnp.sum(g * g) for g in gradients), sum(g.size for g in gradients))
    first = (m_wq, m_wk, m_wv, m_wo, m_w_gate, m_w_up, m_w_down)
    second = (v_wq, v_wk, v_wv, v_wo, v_w_gate, v_w_up, v_w_down)
    new = [adamw(weights[name].astype(jnp.float32), m, v, g) for name, m, v, g in zip(NAMES, first, second, gradients, strict=True)]
    return tuple(one[which] for which in range(3) for one in new)
```

```python
import functools

import jax
import jax.numpy as jnp
from jax import lax
from jax.experimental import pallas as pl
from jax.experimental.pallas import tpu as pltpu
from jax.sharding import PartitionSpec as P

NEG = -1e30
HIDDEN = 2 * NEG
LOG2E = 1.4426950408889634
VMEM = 58 * 2**20
BLOCK = 512
HEAD = 256
THETA = 10000
NAMES = ("wq", "wk", "wv", "wo", "w_gate", "w_up", "w_down")


def _dot(a, b, ca, cb):
    return lax.dot_general(a, b, (((ca,), (cb,)), ((), ())), preferred_element_type=jnp.float32)


def _head(i):
    return slice(i * HEAD, (i + 1) * HEAD)


def _causal():
    return lax.broadcasted_iota(jnp.int32, (BLOCK, BLOCK), 1) >= lax.broadcasted_iota(jnp.int32, (BLOCK, BLOCK), 0)


def _over_blocks(iq, bq, heads, block):
    strips = bq // BLOCK
    whole = [(i, s * BLOCK, False) for i in range(heads) for s in range(strips)]
    lax.fori_loop(0, iq * strips, lambda j, _: block(j, whole), None)
    for t in range(strips):
        block(iq * strips + t, [(i, s * BLOCK, s == t) for i in range(heads) for s in range(t, strips)])


def _forward(q_ref, k_ref, v_ref, o_ref, lse_ref, top_s, mix_s, *, scale):
    bq, heads = q_ref.shape[0], q_ref.shape[1] // HEAD
    iq = pl.program_id(1)
    e = scale * LOG2E
    top_s[...] = jnp.full(top_s.shape, NEG, jnp.float32)
    mix_s[...] = jnp.zeros(mix_s.shape, jnp.float32)
    ones = jnp.ones((8, BLOCK), v_ref.dtype)

    def block(j, pieces):
        here = pl.ds(pl.multiple_of(j * BLOCK, BLOCK), BLOCK)
        scores = [_dot(k_ref[here, _head(i)], q_ref[at : at + BLOCK, _head(i)], 1, 1) for i, at, _ in pieces]
        weights, keeps = [], []
        for (i, at, diagonal), s in zip(pieces, scores):
            if diagonal:
                s = jnp.where(_causal(), s, HIDDEN)
            old = top_s[i : i + 1, at : at + BLOCK]
            top = jnp.maximum(old, s.max(axis=0, keepdims=True))
            top_s[i : i + 1, at : at + BLOCK] = top
            weights.append(jnp.exp2((s - top) * e).astype(v_ref.dtype))
            keeps.append(jnp.exp2((old - top) * e))
        for (i, at, _), p, keep in zip(pieces, weights, keeps):
            values = jnp.concatenate([v_ref[here, _head(i)].T, ones], axis=0)
            mix_s[i, :, at : at + BLOCK] = mix_s[i, :, at : at + BLOCK] * keep + _dot(values, p, 1, 0)

    _over_blocks(iq, bq, heads, block)
    for i in range(heads):
        total = mix_s[i, HEAD : HEAD + 1, :]
        o_ref[:, _head(i)] = (mix_s[i, :HEAD, :] * (1 / total)).T.astype(o_ref.dtype)
        lse_ref[i] = top_s[i : i + 1, :] * scale + jnp.log(total)


def attend(q, k, v, bq=1024, heads=4):
    t, wide = q.shape
    n = wide // HEAD
    mine, keys = pl.BlockSpec((bq, heads * HEAD), lambda ih, iq: (iq, ih)), pl.BlockSpec((t, heads * HEAD), lambda ih, iq: (0, ih))
    return pl.pallas_call(
        functools.partial(_forward, scale=HEAD**-0.5),
        grid=(n // heads, t // bq),
        in_specs=[mine, keys, keys],
        out_specs=[mine, pl.BlockSpec((heads, 1, bq), lambda ih, iq: (ih, 0, iq))],
        scratch_shapes=[pltpu.VMEM((heads, bq), jnp.float32), pltpu.VMEM((heads, HEAD + 8, bq), jnp.float32)],
        out_shape=[jax.ShapeDtypeStruct((t, wide), q.dtype), jax.ShapeDtypeStruct((n, 1, t), jnp.float32)],
        compiler_params=pltpu.CompilerParams(dimension_semantics=("parallel", "parallel"), vmem_limit_bytes=VMEM),
        cost_estimate=pl.CostEstimate(flops=4 * t * t * wide, transcendentals=n * t * t, bytes_accessed=8 * t * wide),
    )(q, k, v)


def _backward(q_ref, k_ref, v_ref, o_ref, do_ref, lse_ref, dq_ref, dk_ref, dv_ref, dq_s, dk_s, dv_s, *, scale):
    bq, heads = q_ref.shape[0], q_ref.shape[1] // HEAD
    iq = pl.program_id(1)
    e = scale * LOG2E

    @pl.when(iq == 0)
    def _():
        dk_s[...] = jnp.zeros_like(dk_s)
        dv_s[...] = jnp.zeros_like(dv_s)

    dq_s[...] = jnp.zeros_like(dq_s)
    lses = [lse_ref[i] * LOG2E for i in range(heads)]
    deltas = [
        (do_ref[:, _head(i)].astype(jnp.float32) * o_ref[:, _head(i)].astype(jnp.float32)).T.sum(axis=0, keepdims=True)
        for i in range(heads)
    ]

    def block(j, pieces):
        here = pl.ds(pl.multiple_of(j * BLOCK, BLOCK), BLOCK)
        qs = [q_ref[at : at + BLOCK, _head(i)] for i, at, _ in pieces]
        dos = [do_ref[at : at + BLOCK, _head(i)] for i, at, _ in pieces]
        scores = [_dot(k_ref[here, _head(i)], x, 1, 1) for (i, _, _), x in zip(pieces, qs)]
        dps = [_dot(v_ref[here, _head(i)], x, 1, 1) for (i, _, _), x in zip(pieces, dos)]
        for n, (i, at, diagonal) in enumerate(pieces):
            p = jnp.exp2(scores[n] * e - lses[i][:, at : at + BLOCK])
            if diagonal:
                p = jnp.where(_causal(), p, 0.0)
            ds = (p * (dps[n] - deltas[i][:, at : at + BLOCK])).astype(q_ref.dtype)
            dv_s[here, _head(i)] += _dot(p.astype(q_ref.dtype), dos[n], 1, 0)
            dk_s[here, _head(i)] += _dot(ds, qs[n], 1, 0)
            dq_s[i, :, at : at + BLOCK] += _dot(k_ref[here, _head(i)].T, ds, 1, 0)

    _over_blocks(iq, bq, heads, block)
    for i in range(heads):
        dq_ref[:, _head(i)] = (dq_s[i] * scale).T.astype(dq_ref.dtype)

    @pl.when(iq == pl.num_programs(1) - 1)
    def _():
        dk_ref[...] = (dk_s[...] * scale).astype(dk_ref.dtype)
        dv_ref[...] = dv_s[...].astype(dv_ref.dtype)


def attend_bwd(q, k, v, out, d_out, lse, bq=1024, heads=2):
    t, wide = q.shape
    n = wide // HEAD
    mine, keys = pl.BlockSpec((bq, heads * HEAD), lambda ih, iq: (iq, ih)), pl.BlockSpec((t, heads * HEAD), lambda ih, iq: (0, ih))
    return pl.pallas_call(
        functools.partial(_backward, scale=HEAD**-0.5),
        grid=(n // heads, t // bq),
        in_specs=[mine, keys, keys, mine, mine, pl.BlockSpec((heads, 1, bq), lambda ih, iq: (ih, 0, iq))],
        out_specs=[mine, keys, keys],
        scratch_shapes=[
            pltpu.VMEM((heads, HEAD, bq), jnp.float32),
            pltpu.VMEM((t, heads * HEAD), jnp.float32),
            pltpu.VMEM((t, heads * HEAD), jnp.float32),
        ],
        out_shape=[jax.ShapeDtypeStruct((t, wide), q.dtype)] * 3,
        compiler_params=pltpu.CompilerParams(dimension_semantics=("parallel", "arbitrary"), vmem_limit_bytes=VMEM),
        cost_estimate=pl.CostEstimate(flops=10 * t * t * wide, transcendentals=n * t * t, bytes_accessed=16 * t * wide),
    )(q, k, v, out, d_out, lse)


def _turn(x_ref, y_ref, cos_ref, sin_ref, xo_ref, yo_ref, *, back):
    cos, sin = cos_ref[...], -sin_ref[...] if back else sin_ref[...]
    half = HEAD // 2
    for ref, to in ((x_ref, xo_ref), (y_ref, yo_ref)):
        for at in range(0, ref.shape[1], HEAD):
            a, b = ref[:, at : at + half].astype(jnp.float32), ref[:, at + half : at + HEAD].astype(jnp.float32)
            to[:, at : at + half] = (a * cos - b * sin).astype(to.dtype)
            to[:, at + half : at + HEAD] = (b * cos + a * sin).astype(to.dtype)


def turned(x, y, cos, sin, back=False):
    t, wide = x.shape
    rows = 512
    data, table = pl.BlockSpec((rows, wide), lambda i: (i, 0)), pl.BlockSpec((rows, HEAD // 2), lambda i: (i, 0))
    return pl.pallas_call(
        functools.partial(_turn, back=back),
        grid=(t // rows,),
        in_specs=[data, data, table, table],
        out_specs=[data, data],
        out_shape=[jax.ShapeDtypeStruct((t, wide), x.dtype)] * 2,
        compiler_params=pltpu.CompilerParams(dimension_semantics=("parallel",), vmem_limit_bytes=24 * 2**20),
        cost_estimate=pl.CostEstimate(flops=12 * t * wide, transcendentals=0, bytes_accessed=9 * t * wide),
    )(x, y, cos, sin)


def _mlp(b_ref, gate_w, up_w, gate_ref, up_ref, act_ref):
    for at in range(0, b_ref.shape[0], BLOCK):
        rows = slice(at, at + BLOCK)
        gate, up = _dot(b_ref[rows, :], gate_w[0], 1, 0), _dot(b_ref[rows, :], up_w[0], 1, 0)
        gate_ref[rows, :] = gate
        up_ref[rows, :] = up
        act_ref[rows, :] = (gate * jax.nn.sigmoid(gate) * up).astype(act_ref.dtype)


def mlp(b, w_gate, w_up, number, columns=256):
    t, d = b.shape
    f = w_gate.shape[2]
    weight, out = pl.BlockSpec((1, d, columns), lambda j: (number, 0, j)), pl.BlockSpec((t, columns), lambda j: (0, j))
    return pl.pallas_call(
        _mlp,
        grid=(f // columns,),
        in_specs=[pl.BlockSpec((t, d), lambda j: (0, 0)), weight, weight],
        out_specs=[out, out, out],
        out_shape=[jax.ShapeDtypeStruct((t, f), dtype) for dtype in (jnp.float32, jnp.float32, b.dtype)],
        compiler_params=pltpu.CompilerParams(dimension_semantics=("parallel",), vmem_limit_bytes=40 * 2**20),
        cost_estimate=pl.CostEstimate(flops=4 * t * d * f, transcendentals=t * f, bytes_accessed=10 * t * f + 4 * d * f),
    )(b, w_gate, w_up)


def _mlp_back(d_ref, down_w, gate_ref, up_ref, d_gate_ref, d_up_ref):
    for at in range(0, d_ref.shape[0], BLOCK):
        rows = slice(at, at + BLOCK)
        d_act = _dot(d_ref[rows, :], down_w[0], 1, 1).astype(d_ref.dtype).astype(jnp.float32)
        gate = gate_ref[rows, :]
        s = jax.nn.sigmoid(gate)
        d_up_ref[rows, :] = (d_act * (gate * s)).astype(d_up_ref.dtype)
        d_gate_ref[rows, :] = (d_act * up_ref[rows, :] * (s * (1 + gate * (1 - s)))).astype(d_gate_ref.dtype)


def mlp_back(d, w_down, gate, up, number, columns=256):
    t, wide = d.shape
    f = w_down.shape[1]
    block = pl.BlockSpec((t, columns), lambda j: (0, j))
    return pl.pallas_call(
        _mlp_back,
        grid=(f // columns,),
        in_specs=[pl.BlockSpec((t, wide), lambda j: (0, 0)), pl.BlockSpec((1, columns, wide), lambda j: (number, j, 0)), block, block],
        out_specs=[block, block],
        out_shape=[jax.ShapeDtypeStruct((t, f), d.dtype)] * 2,
        compiler_params=pltpu.CompilerParams(dimension_semantics=("parallel",), vmem_limit_bytes=40 * 2**20),
        cost_estimate=pl.CostEstimate(flops=2 * t * wide * f, transcendentals=t * f, bytes_accessed=12 * t * f + 2 * wide * f),
    )(d, w_down, gate, up)


def _pair_grad(a_ref, x_ref, y_ref, o_ref, turned_s):
    which, rows = pl.program_id(0), 256
    per = o_ref.shape[1]

    @pl.when((which == 0) & (pl.program_id(1) == 0))
    def _():
        turned_s[...] = a_ref[...].T

    def run(ref):
        for at in range(0, turned_s.shape[0], rows):
            got = _dot(turned_s[at : at + rows, :], ref[...], 1, 0).astype(o_ref.dtype)
            if per <= rows:
                o_ref[at // per : (at + rows) // per] = got.reshape(rows // per, per, -1)
            else:
                o_ref[at // per, at % per : at % per + rows, :] = got

    pl.when(which == 0)(lambda: run(x_ref))
    pl.when(which == 1)(lambda: run(y_ref))


def pair_grad(a, x, y, n, columns=512):
    t, d = a.shape
    f = x.shape[1]
    steps = f // columns
    joined = pl.pallas_call(
        _pair_grad,
        grid=(2, steps),
        in_specs=[
            pl.BlockSpec((t, d), lambda w, j: (0, 0)),
            pl.BlockSpec((t, columns), lambda w, j: (0, j * (1 - w) + (steps - 1) * w)),
            pl.BlockSpec((t, columns), lambda w, j: (0, j * w)),
        ],
        out_specs=pl.BlockSpec((n, d // n, columns), lambda w, j: (0, w, j)),
        out_shape=jax.ShapeDtypeStruct((n, 2 * d // n, f), a.dtype),
        scratch_shapes=[pltpu.VMEM((d, t), a.dtype)],
        compiler_params=pltpu.CompilerParams(dimension_semantics=("arbitrary", "arbitrary"), vmem_limit_bytes=48 * 2**20),
        cost_estimate=pl.CostEstimate(flops=4 * t * d * f, transcendentals=0, bytes_accessed=4 * (t * d + t * f + d * f)),
    )(a, x, y)
    return joined.reshape(2 * d, f)


def _share(n, x_ref, o_ref, slots, send_sem, recv_sem):
    me = lax.axis_index("dp")
    barrier = pltpu.get_barrier_semaphore()
    others = [lax.rem(me + step, n) for step in range(1, n)]
    for other in others:
        pl.semaphore_signal(barrier, inc=1, device_id={"dp": other}, device_id_type=pl.DeviceIdType.MESH)
    pl.semaphore_wait(barrier, n - 1)
    copies = []
    for step, other in enumerate(others):
        copy = pltpu.make_async_remote_copy(
            src_ref=x_ref,
            dst_ref=slots.at[step],
            send_sem=send_sem.at[step],
            recv_sem=recv_sem.at[step],
            device_id={"dp": other},
            device_id_type=pl.DeviceIdType.MESH,
        )
        copy.start()
        copies.append(copy)
    for copy in copies:
        copy.wait()
    total = x_ref[...]
    for step in range(n - 1):
        total = total + slots[step]
    o_ref[...] = total


def summed(x, n):
    tile = jnp.broadcast_to(x, (8, 128))
    spec = pl.BlockSpec(memory_space=pltpu.VMEM)
    total = pl.pallas_call(
        functools.partial(_share, n),
        in_specs=[spec],
        out_specs=spec,
        out_shape=jax.ShapeDtypeStruct((8, 128), jnp.float32),
        scratch_shapes=[pltpu.VMEM((n - 1, 8, 128), jnp.float32), pltpu.SemaphoreType.DMA((n - 1,)), pltpu.SemaphoreType.DMA((n - 1,))],
        compiler_params=pltpu.CompilerParams(collective_id=0, has_side_effects=True),
    )(tile)
    return total[0, 0]


def _pick(x_ref, o_ref):
    o_ref[...] = x_ref[...]


def picked(x, start, rows, layers):
    n, _, columns = x.shape
    per = min(rows, 2**19 // columns)
    cut = rows // per
    return pl.pallas_call(
        _pick,
        grid=(layers, n, cut),
        in_specs=[pl.BlockSpec((1, per, columns), lambda l, i, c: (i, (start + l * rows) // per + c, 0))],
        out_specs=pl.BlockSpec((1, per, columns), lambda l, i, c: (l, i * cut + c, 0)),
        out_shape=jax.ShapeDtypeStruct((layers, n * rows, columns), x.dtype),
        compiler_params=pltpu.CompilerParams(dimension_semantics=("parallel",) * 3, vmem_limit_bytes=16 * 2**20),
        cost_estimate=pl.CostEstimate(flops=layers * n * rows * columns, transcendentals=0, bytes_accessed=4 * layers * n * rows * columns),
    )(x)


def matmul(a, w):
    return jnp.dot(a, w, preferred_element_type=jnp.float32).astype(jnp.bfloat16)


def matmul_t(a, w):
    return _dot(a, w, 1, 1).astype(jnp.bfloat16)


def weight_grad(a, d):
    return _dot(a, d, 0, 0).astype(jnp.bfloat16)


def normed(h):
    wide = h.astype(jnp.float32)
    scale = lax.rsqrt(jnp.mean(wide**2, -1, keepdims=True) + 1e-6)
    return (wide * scale).astype(jnp.bfloat16)


def normed_bwd(h, d):
    return jax.vjp(normed, h)[1](d)[0]


def adamw(w, m, v, g):
    m = 0.9 * m + 0.1 * g
    v = 0.95 * v + 0.05 * g * g
    step = m * lax.rsqrt(v + 1e-8) + 0.1 * w
    return (w - 0.02 * step).astype(jnp.bfloat16), m, v


def forward(h, weights, number, cos, sin):
    w = {name: weights[name][number] for name in ("wq", "wk", "wv", "wo")}
    a = normed(h)
    q, k = turned(matmul(a, w["wq"]), matmul(a, w["wk"]), cos, sin)
    v = matmul(a, w["wv"])
    out, lse = attend(q, k, v)
    h2 = h + matmul(out, w["wo"])
    b = normed(h2)
    gate, up, act = mlp(b, weights["w_gate"], weights["w_up"], number)
    return h2 + matmul(act, weights["w_down"][number]), (h, a, q, k, v, out, lse, h2, b, gate, up, act)


def solution(mesh):
    n = mesh.shape["dp"]

    def joined(parts):
        rows = [g.shape[0] // n for g in parts]
        return jnp.concatenate([g.reshape(n, r, g.shape[1]) for g, r in zip(parts, rows)], axis=1).reshape(-1, parts[0].shape[1])

    def step(x, dy, *arrays):
        weights, m, v = (dict(zip(NAMES, arrays[i : i + 7], strict=True)) for i in (0, 7, 14))
        layers = arrays[0].shape[0]
        half = HEAD // 2
        angle = jnp.arange(x.shape[1], dtype=jnp.float32)[:, None] * THETA ** (-jnp.arange(half, dtype=jnp.float32) / half)
        cos, sin = jnp.cos(angle), jnp.sin(angle)
        of = [{name: w[number] for name, w in weights.items()} for number in range(layers)]
        h, kept = x[0], []
        for number in range(layers):
            h, saved = forward(h, weights, number, cos, sin)
            kept.append(saved)

        d, mine, flights = dy[0], [{} for _ in range(layers)], []
        barrier = lax.optimization_barrier

        def land(flight):
            at = 0
            for number, name, rows in flight[0]:
                mine[number][name] = flight[1][at : at + rows]
                at += rows

        def send(items, *then, flying, whole=None):
            ended, flights[:] = flights[: len(flights) - flying], flights[len(flights) - flying :]
            whole = joined([g for _, _, g in items]) if whole is None else whole
            whole, then, got = barrier((whole, then, [one[1] for one in ended]))
            for (rows, _), array in zip(ended, got):
                land((rows, array))
            flights.append(([(number, name, m[name].shape[1]) for number, name, _ in items],
                            lax.psum_scatter(whole, "dp", scatter_dimension=0, tiled=True)))
            return then

        for number in reversed(range(layers)):
            w = of[number]
            h, a, q, k, val, out, lse, h2, b, gate, up, act = kept[number]
            (d,) = send([(number, "w_down", weight_grad(act, d))], d, flying=min(len(flights), 1))
            d_gate, d_up = mlp_back(d, weights["w_down"], gate, up, number)
            d_gate, d_up = send([(number, "w_gate", None), (number, "w_up", None)], d_gate, d_up, flying=1, whole=pair_grad(b, d_gate, d_up, n))
            d = d + normed_bwd(h2, matmul_t(d_gate, w["w_gate"]) + matmul_t(d_up, w["w_up"]))
            g_o = weight_grad(out, d)
            dq, dk, dv = attend_bwd(q, k, val, out, matmul_t(d, w["wo"]), lse)
            dq, dk = turned(dq, dk, cos, sin, back=True)
            items = [(number, "wq", weight_grad(a, dq)), (number, "wk", weight_grad(a, dk)), (number, "wv", weight_grad(a, dv)), (number, "wo", g_o)]
            dq, dk, dv = send(items, dq, dk, dv, flying=1 if number else 0)
            if number:
                d = d + normed_bwd(h, matmul_t(dq, w["wq"]) + matmul_t(dk, w["wk"]) + matmul_t(dv, w["wv"]))
        land(flights[0])

        gradients = {name: jnp.stack([mine[number][name] for number in range(layers)]).astype(jnp.float32) for name in NAMES}
        squares = summed(sum(jnp.sum(g * g) for g in gradients.values()), n)
        count = n * sum(g.size for g in gradients.values())
        factor = jnp.minimum(1.0, 0.5 * lax.rsqrt(squares / count + 1e-30))
        me = lax.axis_index("dp")
        new = {}
        for name in NAMES:
            rows = m[name].shape[1]
            own = lax.dynamic_slice_in_dim(weights[name], me * rows, rows, 1).astype(jnp.float32)
            new[name] = adamw(own, m[name], v[name], gradients[name] * factor)

        whole = {}
        for names in (("w_gate", "w_up"), ("w_down", "wq", "wk", "wv", "wo")):
            parts = [new[name][0] for name in names]
            columns = parts[0].shape[2]
            got = lax.all_gather(jnp.concatenate([p.reshape(-1, columns) for p in parts]), "dp", axis=0)
            at = 0
            for name, p in zip(names, parts):
                whole[name] = picked(got, at, p.shape[1], layers)
                at += layers * p.shape[1]
        return (*(whole[name] for name in NAMES), *(new[name][1] for name in NAMES), *(new[name][2] for name in NAMES))

    states, all_of, cut = P(("rep", "dp"), None, None), P(None, None, None), P(None, "dp", None)
    return jax.shard_map(
        step,
        mesh=mesh,
        in_specs=(states, states) + (all_of,) * 7 + (cut,) * 14,
        out_specs=(P("rep", None, None),) * 7 + (P("rep", "dp", None),) * 14,
        check_vma=False,
    )
```
